32 devices in a mesh: dp: 8 (over z, x), ctx: 4 (over y, core).
Axes of the slice: x: 2, y: 2, z: 4, core: 2. Of those that a mesh axis runs over, the one named last changes fastest.
Arguments:
- queries: bfloat16 [8, 1024, 2048], P('dp', 'ctx'), may hold values from -100 to 100
- keys: bfloat16 [8, 1024, 512], P('dp', 'ctx'), may hold values from -4 to 4
- values: bfloat16 [8, 1024, 512], P('dp', 'ctx'), may hold values from -6 to 6
- segments: int32 [8, 1024], P('dp', 'ctx'), may hold values from 0 to 7, never falling along the last dimension, each value on 1 to 512 neighbouring positions
Outputs:
- attended: bfloat16 [8, 1024, 2048], P('dp', 'ctx')
The draws below stay inside these ranges and needn't reach their ends.
Inputs may be any that keep to these rules, and one draw needn't show every extreme that they name: `segments`: document numbers never fall along a packed batch, every one of the 8 documents is present, and each document has at most 512 tokens; some document has exactly 512.
All inputs are finite; a program needn't handle non-finite values.
Results may differ from the reference program's by a relative error of at most 0.0053.
Values may be sent and summed in bfloat16 or wider, within the bound.
A program may use at most 192 MiB of HBM per device.

```python
import math
import jax
import jax.numpy as jnp
import numpy as np
from jax import lax

HQ = 16
HK = 4
HD = 128
SEQ_COUNT = 8
TOKENS = 1024
MOST = 512
N_DP = 8


def draw_pair(key):
    key_keys = jax.random.fold_in(key, 12)
    key_queries = jax.random.fold_in(key, 11)
    key_rows = jnp.clip(jax.random.normal(key_keys, (N_DP, TOKENS, HK * HD), jnp.float32), -4.0, 4.0)
    query_rows = jnp.clip(jax.random.normal(key_queries, (N_DP, TOKENS, HQ * HD), jnp.float32), -4.0, 4.0)
    return (query_rows, key_rows)


def draw_queries(key, part):
    return draw_pair(key)[0].astype(jnp.bfloat16)


def draw_keys(key, part):
    return draw_pair(key)[1].astype(jnp.bfloat16)


def level_of(rng, shape, cuts, smallest, largest):
    factor_of = 1.0
    for dim, blocks in cuts:
        draws = jax.random.uniform(jax.random.fold_in(jax.random.fold_in(rng, 6), dim), (blocks,), jnp.float32, smallest / len(cuts), largest / len(cuts))
        factor_of = factor_of * jnp.repeat(jnp.exp(draws), shape[dim] // blocks).reshape((-1,) + (1,) * (len(shape) - 1 - dim))
    return factor_of


def length_profile(number_of, total, bound, skew):
    loads = [(1 << 20) // math.isqrt(grade ** skew) + 1 for grade in range(2, number_of + 1)]
    spare, counts = total - bound - (number_of - 1), [1] * (number_of - 1)
    while spare > 0:
        movable = [i for i in range(number_of - 1) if counts[i] < bound]
        whole, left = sum([loads[i] for i in movable]), spare
        for i in movable:
            addition = min(bound - counts[i], max(1, left * loads[i] // whole), spare)
            counts[i] = counts[i] + addition
            spare = spare - addition
    return np.array([bound] + counts)


def ragged(own_key, number_of, total, reach, skew):
    if number_of == 2:
        one = jax.random.randint(own_key, (), max(1, total - reach), min(reach, total - 1) + 1)
        return jnp.stack([one, total - one])
    sizes = jnp.asarray(length_profile(number_of, total, reach, skew), jnp.int32)
    pairs = (number_of - 1) // 2
    giver, receiver = sizes[1:1 + 2 * pairs:2], sizes[2:2 + 2 * pairs:2]
    slack = jnp.minimum(giver - 1, reach - receiver)
    moved = jax.random.randint(jax.random.fold_in(own_key, 1), (pairs,), 0, 1 << 20) % (slack + 1)
    sizes = sizes.at[1:1 + 2 * pairs:2].set(giver - moved).at[2:2 + 2 * pairs:2].set(receiver + moved)
    return sizes[jax.random.permutation(jax.random.fold_in(own_key, 2), number_of)]


def scatter_about(stream_key, extent, scale, bound, cuts=(), held_as=jnp.bfloat16):
    entries = jax.random.normal(stream_key, extent, jnp.float32) * scale
    if len(cuts) > 0:
        entries = level_of(stream_key, extent, cuts, -0.22, 0.18) * entries
    return jnp.clip(entries, min=-bound, max=bound).astype(held_as)


def setup_inputs(seed: int = 0) -> dict:
    streams_of = jax.random.split(jax.random.key(seed), 5)
    queries = draw_queries(jax.random.fold_in(streams_of[4], 71), 0)
    keys = draw_keys(jax.random.fold_in(streams_of[4], 71), 0)
    values = scatter_about(streams_of[2], (N_DP, TOKENS, HK * HD), 1.0, 6.0, ((0, 8), (1, 4)))
    segments = jax.vmap(lambda own: jnp.searchsorted(jnp.cumsum(ragged(own, SEQ_COUNT, TOKENS, MOST, 2)), jnp.arange(TOKENS), side="right"))(jax.random.split(streams_of[3], N_DP)).reshape((N_DP, TOKENS)).astype(jnp.int32)
    return dict(queries=queries, keys=keys, values=values, segments=segments)


rope_theta = 500000.0

def rotate(values_in, positions, heads):
    rows = values_in.shape[0]
    half_dim = HD // 2
    split = values_in.astype(jnp.float32).reshape(rows, heads, HD)
    inv_freq = jnp.exp(-jnp.log(rope_theta) * 2.0 * jnp.arange(half_dim, dtype=jnp.float32) / HD)
    angles = positions.astype(jnp.float32)[:, None] * inv_freq[None, :]
    cosine_part = jnp.cos(angles)[:, None, :]
    sine_part = jnp.sin(angles)[:, None, :]
    first_half = split[..., :half_dim]
    second_half = split[..., half_dim:]
    turned = jnp.concatenate([first_half * cosine_part - second_half * sine_part, second_half * cosine_part + first_half * sine_part], axis=-1)
    return turned.reshape(rows, heads * HD).astype(jnp.bfloat16)

def doc_positions(seg_ids):
    index_all = jnp.arange(seg_ids.shape[0], dtype=jnp.int32)
    previous = jnp.concatenate([seg_ids[:1] - 1, seg_ids[:-1]])
    run_start = lax.cummax(jnp.where(seg_ids != previous, index_all, 0), axis=0)
    return index_all - run_start

def one_batch(inputs):
    query_rows, key_rows, value_rows, seg_ids = inputs
    positions = doc_positions(seg_ids)
    rot_q = rotate(query_rows, positions, HQ)
    rot_k = rotate(key_rows, positions, HK)
    block_rows = min(512, TOKENS)
    pieces = []
    for block_index in range(TOKENS // block_rows):
        q_lo = block_index * block_rows
        key_lo = max(0, q_lo - MOST)
        key_hi = q_lo + block_rows
        width = key_hi - key_lo
        query_heads = rot_q[q_lo:key_hi].astype(jnp.float32).reshape(block_rows, HK, HQ // HK, HD)
        key_heads = rot_k[key_lo:key_hi].astype(jnp.float32).reshape(width, HK, HD)
        value_heads = value_rows[key_lo:key_hi].astype(jnp.float32).reshape(width, HK, HD)
        q_index = q_lo + jnp.arange(block_rows, dtype=jnp.int32)
        k_index = key_lo + jnp.arange(width, dtype=jnp.int32)
        live_mask = (seg_ids[key_lo:key_hi][None, :] == seg_ids[q_lo:key_hi][:, None]) & (k_index[None, :] <= q_index[:, None])
        scores = jnp.einsum('thgd,shd->hgts', query_heads, key_heads) / jnp.sqrt(jnp.float32(HD))
        scores = jnp.where(live_mask, scores, jnp.float32(-1e+30))
        row_max = lax.optimization_barrier(jnp.max(scores, axis=-1, keepdims=True))
        weights = jnp.where(live_mask, jnp.exp(scores - row_max), jnp.float32(0.0))
        denom = lax.optimization_barrier(jnp.sum(weights, axis=-1))
        rounded = lax.optimization_barrier(weights.astype(jnp.bfloat16)).astype(jnp.float32)
        weighted = jnp.einsum('hgts,shd->thgd', rounded, value_heads)
        result = weighted / jnp.transpose(denom, (2, 0, 1))[..., None]
        pieces.append(result.reshape(block_rows, HQ * HD).astype(jnp.bfloat16))
    return jnp.concatenate(pieces, axis=0)

def reference(queries, keys, values, segments):
    attended = lax.map(one_batch, (queries, keys, values, segments))
    return attended
```

```python
import functools
import math

import jax
import jax.numpy as jnp
from jax import lax
from jax.experimental import pallas as pl
from jax.experimental.pallas import tpu as pltpu
from jax.sharding import PartitionSpec as P

HK = 4
HD = 128
THETA = 500000.0
LANES = 128
MASKED = -1e30
F32 = jnp.float32
BF16 = jnp.bfloat16


def sin_cos(angle):
    turns = jnp.floor(angle * (2.0 / math.pi) + 0.5)
    rest = angle - turns * 1.5703125
    rest = rest - turns * 4.837512969970703125e-4
    rest = rest - turns * 7.54978995489188216e-8
    square = rest * rest
    sine = rest + rest * square * (
        -1.6666654611e-1 + square * (8.3321608736e-3 + square * -1.9515295891e-4)
    )
    cosine = (
        1.0
        - 0.5 * square
        + square * square * (4.166664568298827e-2 + square * (-1.388731625493765e-3 + square * 2.443315711809948e-5))
    )
    quarter = turns - 4.0 * jnp.floor(turns * 0.25)
    odd = (quarter == 1.0) | (quarter == 3.0)
    sin_out = jnp.where(odd, cosine, sine)
    cos_out = jnp.where(odd, sine, cosine)
    sin_out = jnp.where(quarter >= 2.0, -sin_out, sin_out)
    cos_out = jnp.where((quarter == 1.0) | (quarter == 2.0), -cos_out, cos_out)
    return sin_out, cos_out


def frequencies():
    index = lax.broadcasted_iota(jnp.int32, (1, HD), 1) % (HD // 2)
    result = jnp.ones((1, HD), F32)
    bit = 1
    while bit < HD // 2:
        factor = math.exp(-math.log(THETA) * 2.0 * bit / HD)
        result = result * jnp.where((index // bit) % 2 == 1, F32(factor), F32(1.0))
        bit *= 2
    return result


def turned(block, cosine, sine):
    block = block.astype(F32)
    return (block * cosine + pltpu.roll(block, HD // 2, 1) * sine).astype(BF16)


def kernel(
    count, hops, q_ref, k_ref, v_ref, seg_ref, out_ref,
    q_own, kwin, vwin, segwin, krot, qrot, weights, denoms, sines, cosines, bias,
    q_sem, seg_sem, own_sem, seg_send, seg_recv, send, recv, forward,
):
    me = lax.axis_index("ctx")
    rows = q_own.shape[0]
    width = kwin.shape[1]
    group = qrot.shape[0] // HK
    windows = (kwin, vwin)

    def block(which, head, distance):
        return windows[which].at[head, pl.ds((hops - distance) * rows, rows)]

    own_copies = [
        [
            pltpu.make_async_copy(
                ref.at[0, :, pl.ds(head * HD, HD)], block(which, head, 0), own_sem.at[which, head]
            )
            for head in range(HK)
        ]
        for which, ref in enumerate((k_ref, v_ref))
    ]
    seg_copy = pltpu.make_async_copy(seg_ref, segwin.at[hops], seg_sem)
    q_copy = pltpu.make_async_copy(q_ref.at[0], q_own, q_sem)
    seg_copy.start()
    for head in range(HK):
        for which in range(2):
            own_copies[which][head].start()
    q_copy.start()

    barrier = pltpu.get_barrier_semaphore()
    for distance in range(1, hops + 1):
        @pl.when(me + distance < count)
        def _():
            pl.semaphore_signal(barrier, inc=1, device_id={"ctx": me + distance})

        @pl.when(me >= distance)
        def _():
            pl.semaphore_signal(barrier, inc=1, device_id={"ctx": me - distance})
    pl.semaphore_wait(barrier, jnp.minimum(me, hops) + jnp.minimum(count - 1 - me, hops))

    def seg_out(distance):
        return pltpu.make_async_remote_copy(
            src_ref=segwin.at[hops], dst_ref=segwin.at[hops - distance],
            send_sem=seg_send.at[distance - 1], recv_sem=seg_recv.at[distance - 1],
            device_id={"ctx": me + distance},
        )

    def block_out(which, head, distance):
        return pltpu.make_async_remote_copy(
            src_ref=block(which, head, 0), dst_ref=block(which, head, distance),
            send_sem=send.at[which, head, distance - 1], recv_sem=recv.at[which, head, distance - 1],
            device_id={"ctx": me + distance},
        )

    def block_on(which, head, distance):
        return pltpu.make_async_remote_copy(
            src_ref=block(which, head, distance), dst_ref=block(which, head, distance + 1),
            send_sem=forward.at[which, head, distance - 1], recv_sem=recv.at[which, head, distance],
            device_id={"ctx": me + 1},
        )

    def goes_out(distance):
        direct = me + distance < count
        if distance > 1:
            direct = direct & ((me + distance) % 2 == 0)
        return direct

    def goes_on(distance):
        return (me % 2 == 0) & (me >= distance) & (me + 1 < count)

    seg_copy.wait()
    for distance in range(1, hops + 1):
        @pl.when(me + distance < count)
        def _():
            seg_out(distance).start()
    for head in range(HK):
        for which in range(2):
            own_copies[which][head].wait()
            for distance in range(hops, 0, -1):
                @pl.when(goes_out(distance))
                def _():
                    block_out(which, head, distance).start()

    for distance in range(1, hops + 1):
        @pl.when(me < distance)
        def _():
            empty = jnp.zeros((HK, rows, HD), BF16)
            kwin[:, pl.ds((hops - distance) * rows, rows)] = empty
            vwin[:, pl.ds((hops - distance) * rows, rows)] = empty
            segwin[hops - distance] = jnp.full((1, rows), -1, jnp.int32)

    for distance in range(1, hops + 1):
        @pl.when(me >= distance)
        def _():
            seg_out(distance).wait_recv()

    freq = frequencies()
    lane = lax.broadcasted_iota(jnp.int32, (rows, LANES), 1)
    row = lax.broadcasted_iota(jnp.int32, (rows, LANES), 0)
    sign = jnp.where(lane < HD // 2, F32(-1.0), F32(1.0))
    ones = jnp.ones((LANES, LANES), BF16)
    pieces = []
    for index in range(hops + 1):
        seg_row = segwin[index].astype(F32)
        pieces += [seg_row[:, at:at + LANES] for at in range(0, rows, LANES)]
    for index in range(hops + 1):
        column = jnp.broadcast_to(segwin[index].astype(F32), (LANES, rows)).T
        smaller = jnp.zeros((rows, LANES), F32)
        for piece in pieces:
            smaller = smaller + jnp.where(piece < column, F32(1.0), F32(0.0))
        start = jnp.dot(smaller.astype(BF16), ones, preferred_element_type=F32)
        position = (row + index * rows).astype(F32) - start
        sine, cosine = sin_cos(position * freq)
        sines[index] = sine * sign
        cosines[index] = cosine
        if index == hops:
            last = (row + hops * rows).astype(F32)
            for at in range(0, width, LANES):
                spot = (lane + at).astype(F32)
                bias[:, at:at + LANES] = jnp.where(
                    (spot >= start) & (spot <= last), F32(0.0), F32(MASKED)
                )

    q_copy.wait()

    @pl.loop(0, qrot.shape[0])
    def _(head):
        at = pl.ds(pl.multiple_of(head * HD, HD), HD)
        qrot[head] = turned(q_own[:, at], cosines[hops], sines[hops])

    scale = F32(math.log2(math.e) / math.sqrt(HD))

    def arrive(which, head):
        for distance in range(1, hops + 1):
            @pl.when(me >= distance)
            def _():
                block_out(which, head, distance).wait_recv()
            if distance < hops:
                @pl.when(goes_on(distance))
                def _():
                    block_on(which, head, distance).start()

    @pl.loop(0, HK)
    def _(head):
        arrive(0, head)
        for index in range(hops + 1):
            at = pl.ds(index * rows, rows)
            krot[at] = turned(kwin[head, at], cosines[index], sines[index])

        @pl.loop(0, group)
        def _(part):
            scores = lax.dot_general(
                qrot[head * group + part], krot[...], (((1,), (1,)), ((), ())),
                preferred_element_type=F32,
            ) + bias[...]
            top = jnp.max(scores, axis=1, keepdims=True)
            weight = jnp.exp2((scores - top) * scale)
            denoms[part] = jnp.broadcast_to(jnp.sum(weight, axis=1, keepdims=True), (rows, LANES))
            weights[part] = weight.astype(BF16)

        arrive(1, head)

        @pl.loop(0, group)
        def _(part):
            total = jnp.dot(weights[part], vwin[head], preferred_element_type=F32)
            at = pl.ds(pl.multiple_of((head * group + part) * HD, HD), HD)
            out_ref[0, :, at] = (total / denoms[part]).astype(BF16)

    for distance in range(1, hops + 1):
        @pl.when(me + distance < count)
        def _():
            seg_out(distance).wait_send()
        for which in range(2):
            for head in range(HK):
                @pl.when(goes_out(distance))
                def _():
                    block_out(which, head, distance).wait_send()
                if distance < hops:
                    @pl.when(goes_on(distance))
                    def _():
                        block_on(which, head, distance).wait_send()


def body(queries, keys, values, segments):
    count = lax.axis_size("ctx")
    hops = count // 2
    rows = queries.shape[1]
    width = (hops + 1) * rows
    heads = queries.shape[2] // HD
    group = heads // HK
    anywhere = pl.BlockSpec(memory_space=pltpu.HBM)
    dma = pltpu.SemaphoreType.DMA
    return pl.pallas_call(
        functools.partial(kernel, count, hops),
        out_shape=jax.ShapeDtypeStruct(queries.shape, BF16),
        in_specs=[anywhere] * 4,
        out_specs=pl.BlockSpec(memory_space=pltpu.VMEM),
        scratch_shapes=[
            pltpu.VMEM((rows, heads * HD), BF16),
            pltpu.VMEM((HK, width, HD), BF16),
            pltpu.VMEM((HK, width, HD), BF16),
            pltpu.VMEM((hops + 1, 1, rows), jnp.int32),
            pltpu.VMEM((width, HD), BF16),
            pltpu.VMEM((heads, rows, HD), BF16),
            pltpu.VMEM((group, rows, width), BF16),
            pltpu.VMEM((group, rows, LANES), F32),
            pltpu.VMEM((hops + 1, rows, HD), F32),
            pltpu.VMEM((hops + 1, rows, HD), F32),
            pltpu.VMEM((rows, width), F32),
            dma, dma, dma((2, HK)),
            dma((hops,)), dma((hops,)),
            dma((2, HK, hops)), dma((2, HK, hops)), dma((2, HK, hops)),
        ],
        compiler_params=pltpu.CompilerParams(
            collective_id=0, has_side_effects=True, vmem_limit_bytes=48 * 1024 * 1024
        ),
        name="attend",
    )(queries, keys, values, segments)


def solution(mesh):
    placed = (P("dp", "ctx", None), P("dp", "ctx", None), P("dp", "ctx", None), P("dp", "ctx"))
    return jax.shard_map(
        body, mesh=mesh, in_specs=placed, out_specs=P("dp", "ctx", None), check_vma=False
    )
```

```python
import functools
import math

import jax
import jax.numpy as jnp
from jax import lax
from jax.experimental import pallas as pl
from jax.experimental.pallas import tpu as pltpu
from jax.sharding import PartitionSpec as P

HK = 4
HD = 128
THETA = 500000.0
LANES = 128
MASKED = -1e30
F32 = jnp.float32
BF16 = jnp.bfloat16


def sin_cos(angle):
    turns = jnp.floor(angle * (2.0 / math.pi) + 0.5)
    rest = angle - turns * 1.5703125
    rest = rest - turns * 4.837512969970703125e-4
    rest = rest - turns * 7.54978995489188216e-8
    square = rest * rest
    sine = rest + rest * square * (
        -1.6666654611e-1 + square * (8.3321608736e-3 + square * -1.9515295891e-4)
    )
    cosine = (
        1.0
        - 0.5 * square
        + square * square * (4.166664568298827e-2 + square * (-1.388731625493765e-3 + square * 2.443315711809948e-5))
    )
    quarter = turns - 4.0 * jnp.floor(turns * 0.25)
    odd = (quarter == 1.0) | (quarter == 3.0)
    sin_out = jnp.where(odd, cosine, sine)
    cos_out = jnp.where(odd, sine, cosine)
    sin_out = jnp.where(quarter >= 2.0, -sin_out, sin_out)
    cos_out = jnp.where((quarter == 1.0) | (quarter == 2.0), -cos_out, cos_out)
    return sin_out, cos_out


def frequencies():
    index = lax.broadcasted_iota(jnp.int32, (1, HD), 1) % (HD // 2)
    result = jnp.ones((1, HD), F32)
    bit = 1
    while bit < HD // 2:
        factor = math.exp(-math.log(THETA) * 2.0 * bit / HD)
        result = result * jnp.where((index // bit) % 2 == 1, F32(factor), F32(1.0))
        bit *= 2
    return result


def turned(block, cosine, sine):
    block = block.astype(F32)
    return (block * cosine + pltpu.roll(block, HD // 2, 1) * sine).astype(BF16)


def kernel(
    count, hops, q_ref, k_ref, v_ref, seg_ref, out_ref,
    q_own, kwin, vwin, segwin, krot, qrot, weights, denoms, sines, cosines, bias,
    q_sem, seg_sem, own_sem, seg_send, seg_recv, send, recv, forward,
):
    me = lax.axis_index("ctx")
    rows = q_own.shape[0]
    span = bias.shape[2]
    group = qrot.shape[0] // HK
    windows = (kwin, vwin)

    def block(which, head, distance):
        return windows[which].at[head, pl.ds((hops - distance) * rows, rows)]

    own_copies = [
        [
            pltpu.make_async_copy(
                ref.at[0, :, pl.ds(head * HD, HD)], block(which, head, 0), own_sem.at[which, head]
            )
            for head in range(HK)
        ]
        for which, ref in enumerate((k_ref, v_ref))
    ]
    seg_copy = pltpu.make_async_copy(seg_ref, segwin.at[hops], seg_sem)
    q_copy = pltpu.make_async_copy(q_ref.at[0], q_own, q_sem)
    seg_copy.start()
    for head in range(HK):
        for which in range(2):
            own_copies[which][head].start()
    q_copy.start()

    barrier = pltpu.get_barrier_semaphore()
    for distance in range(1, hops + 1):
        @pl.when(me + distance < count)
        def _():
            pl.semaphore_signal(barrier, inc=1, device_id={"ctx": me + distance})

        @pl.when(me >= distance)
        def _():
            pl.semaphore_signal(barrier, inc=1, device_id={"ctx": me - distance})
    pl.semaphore_wait(barrier, jnp.minimum(me, hops) + jnp.minimum(count - 1 - me, hops))

    def seg_out(distance):
        return pltpu.make_async_remote_copy(
            src_ref=segwin.at[hops], dst_ref=segwin.at[hops - distance],
            send_sem=seg_send.at[distance - 1], recv_sem=seg_recv.at[distance - 1],
            device_id={"ctx": me + distance},
        )

    def block_out(which, head, distance):
        return pltpu.make_async_remote_copy(
            src_ref=block(which, head, 0), dst_ref=block(which, head, distance),
            send_sem=send.at[which, head, distance - 1], recv_sem=recv.at[which, head, distance - 1],
            device_id={"ctx": me + distance},
        )

    def block_on(which, head, distance):
        return pltpu.make_async_remote_copy(
            src_ref=block(which, head, distance), dst_ref=block(which, head, distance + 1),
            send_sem=forward.at[which, head, distance - 1], recv_sem=recv.at[which, head, distance],
            device_id={"ctx": me + 1},
        )

    def goes_out(distance):
        direct = me + distance < count
        if distance > 1:
            direct = direct & ((me + distance) % 2 == 0)
        return direct

    def goes_on(distance):
        return (me % 2 == 0) & (me >= distance) & (me + 1 < count)

    seg_copy.wait()
    for distance in range(1, hops + 1):
        @pl.when(me + distance < count)
        def _():
            seg_out(distance).start()
    for head in range(HK):
        for which in range(2):
            own_copies[which][head].wait()

            @pl.when(goes_out(1))
            def _():
                block_out(which, head, 1).start()
    for distance in range(2, hops + 1):
        @pl.when(goes_out(distance))
        def _():
            for head in range(HK):
                for which in range(2):
                    if distance == 2:
                        block_out(which, head, 1).wait_send()
                    block_out(which, head, distance).start()

    for distance in range(1, hops + 1):
        @pl.when(me < distance)
        def _():
            empty = jnp.zeros((HK, rows, HD), BF16)
            kwin[:, pl.ds((hops - distance) * rows, rows)] = empty
            vwin[:, pl.ds((hops - distance) * rows, rows)] = empty
            segwin[hops - distance] = jnp.full((1, rows), -1, jnp.int32)

    for distance in range(1, hops + 1):
        @pl.when(me >= distance)
        def _():
            seg_out(distance).wait_recv()

    freq = frequencies()
    lane = lax.broadcasted_iota(jnp.int32, (rows, LANES), 1)
    row = lax.broadcasted_iota(jnp.int32, (rows, LANES), 0)
    sign = jnp.where(lane < HD // 2, F32(-1.0), F32(1.0))
    ones = jnp.ones((LANES, LANES), BF16)
    pieces = []
    for index in range(hops + 1):
        seg_row = segwin[index].astype(F32)
        pieces += [seg_row[:, at:at + LANES] for at in range(0, rows, LANES)]
    for index in range(hops + 1):
        column = jnp.broadcast_to(segwin[index].astype(F32), (LANES, rows)).T
        smaller = jnp.zeros((rows, LANES), F32)
        for piece in pieces:
            smaller = smaller + jnp.where(piece < column, F32(1.0), F32(0.0))
        start = jnp.dot(smaller.astype(BF16), ones, preferred_element_type=F32)
        position = (row + index * rows).astype(F32) - start
        sine, cosine = sin_cos(position * freq)
        sines[index] = sine * sign
        cosines[index] = cosine
        if index == hops:
            last = (row + hops * rows).astype(F32)
            for tile in range(rows // LANES):
                mine = slice(tile * LANES, (tile + 1) * LANES)
                for at in range(0, span, LANES):
                    spot = (lane[mine] + (at + tile * LANES)).astype(F32)
                    bias[tile, :, at:at + LANES] = jnp.where(
                        (spot >= start[mine]) & (spot <= last[mine]), F32(0.0), F32(MASKED)
                    )

    q_copy.wait()

    @pl.loop(0, qrot.shape[0])
    def _(head):
        at = pl.ds(pl.multiple_of(head * HD, HD), HD)
        qrot[head] = turned(q_own[:, at], cosines[hops], sines[hops])

    scale = F32(math.log2(math.e) / math.sqrt(HD))

    def arrive(head, distance, which):
        @pl.when(me >= distance)
        def _():
            block_out(which, head, distance).wait_recv()
        if distance < hops:
            @pl.when(goes_on(distance))
            def _():
                block_on(which, head, distance).start()

    @pl.loop(0, HK)
    def _(head):
        for distance in range(1, hops):
            for which in range(2):
                arrive(head, distance, which)
        arrive(head, hops, 0)
        for index in range(hops + 1):
            at = pl.ds(index * rows, rows)
            krot[at] = turned(kwin[head, at], cosines[index], sines[index])

        for part in range(group):
            for tile in range(rows // LANES):
                mine = slice(tile * LANES, (tile + 1) * LANES)
                seen = pl.ds(tile * LANES, span)
                scores = lax.dot_general(
                    qrot[head * group + part, mine], krot[seen], (((1,), (1,)), ((), ())),
                    preferred_element_type=F32,
                ) + bias[tile]
                top = jnp.max(scores, axis=1, keepdims=True)
                weight = jnp.exp2((scores - top) * scale)
                denoms[part, mine] = jnp.broadcast_to(
                    jnp.sum(weight, axis=1, keepdims=True), (LANES, LANES)
                )
                weights[part, mine] = weight.astype(BF16)

        arrive(head, hops, 1)

        for part in range(group):
            for tile in range(rows // LANES):
                mine = slice(tile * LANES, (tile + 1) * LANES)
                seen = pl.ds(tile * LANES, span)
                total = jnp.dot(weights[part, mine], vwin[head, seen], preferred_element_type=F32)
                at = pl.ds(pl.multiple_of((head * group + part) * HD, HD), HD)
                out_ref[0, mine, at] = (total / denoms[part, mine]).astype(BF16)

    for distance in range(1, hops + 1):
        @pl.when(me + distance < count)
        def _():
            seg_out(distance).wait_send()
        unsent = goes_out(distance)
        if distance == 1 and hops > 1:
            unsent = unsent & jnp.logical_not(goes_out(2))
        for which in range(2):
            for head in range(HK):
                @pl.when(unsent)
                def _():
                    block_out(which, head, distance).wait_send()
                if distance < hops:
                    @pl.when(goes_on(distance))
                    def _():
                        block_on(which, head, distance).wait_send()


def body(queries, keys, values, segments):
    count = lax.axis_size("ctx")
    hops = count // 2
    rows = queries.shape[1]
    width = (hops + 1) * rows
    span = hops * rows + LANES
    heads = queries.shape[2] // HD
    group = heads // HK
    anywhere = pl.BlockSpec(memory_space=pltpu.HBM)
    dma = pltpu.SemaphoreType.DMA
    return pl.pallas_call(
        functools.partial(kernel, count, hops),
        out_shape=jax.ShapeDtypeStruct(queries.shape, BF16),
        in_specs=[anywhere] * 4,
        out_specs=pl.BlockSpec(memory_space=pltpu.VMEM),
        scratch_shapes=[
            pltpu.VMEM((rows, heads * HD), BF16),
            pltpu.VMEM((HK, width, HD), BF16),
            pltpu.VMEM((HK, width, HD), BF16),
            pltpu.VMEM((hops + 1, 1, rows), jnp.int32),
            pltpu.VMEM((width, HD), BF16),
            pltpu.VMEM((heads, rows, HD), BF16),
            pltpu.VMEM((group, rows, span), BF16),
            pltpu.VMEM((group, rows, LANES), F32),
            pltpu.VMEM((hops + 1, rows, HD), F32),
            pltpu.VMEM((hops + 1, rows, HD), F32),
            pltpu.VMEM((rows // LANES, LANES, span), F32),
            dma, dma, dma((2, HK)),
            dma((hops,)), dma((hops,)),
            dma((2, HK, hops)), dma((2, HK, hops)), dma((2, HK, hops)),
        ],
        compiler_params=pltpu.CompilerParams(
            collective_id=0, has_side_effects=True, vmem_limit_bytes=63 * 1024 * 1024
        ),
        name="attend",
    )(queries, keys, values, segments)


def solution(mesh):
    placed = (P("dp", "ctx", None), P("dp", "ctx", None), P("dp", "ctx", None), P("dp", "ctx"))
    return jax.shard_map(
        body, mesh=mesh, in_specs=placed, out_specs=P("dp", "ctx", None), check_vma=False
    )
```

```python
import functools
import math

import jax
import jax.numpy as jnp
from jax import lax
from jax.experimental import pallas as pl
from jax.experimental.pallas import tpu as pltpu
from jax.sharding import PartitionSpec as P

HK = 4
HD = 128
THETA = 500000.0
LANES = 128
MASKED = -1e30
F32 = jnp.float32
BF16 = jnp.bfloat16


def sin_cos(angle):
    turns = jnp.floor(angle * (2.0 / math.pi) + 0.5)
    rest = angle - turns * 1.5703125
    rest = rest - turns * 4.837512969970703125e-4
    rest = rest - turns * 7.54978995489188216e-8
    square = rest * rest
    sine = rest + rest * square * (
        -1.6666654611e-1 + square * (8.3321608736e-3 + square * -1.9515295891e-4)
    )
    cosine = (
        1.0
        - 0.5 * square
        + square * square * (4.166664568298827e-2 + square * (-1.388731625493765e-3 + square * 2.443315711809948e-5))
    )
    quarter = turns - 4.0 * jnp.floor(turns * 0.25)
    odd = (quarter == 1.0) | (quarter == 3.0)
    sin_out = jnp.where(odd, cosine, sine)
    cos_out = jnp.where(odd, sine, cosine)
    sin_out = jnp.where(quarter >= 2.0, -sin_out, sin_out)
    cos_out = jnp.where((quarter == 1.0) | (quarter == 2.0), -cos_out, cos_out)
    return sin_out, cos_out


def frequencies():
    index = lax.broadcasted_iota(jnp.int32, (1, HD), 1) % (HD // 2)
    result = jnp.ones((1, HD), F32)
    bit = 1
    while bit < HD // 2:
        factor = math.exp(-math.log(THETA) * 2.0 * bit / HD)
        result = result * jnp.where((index // bit) % 2 == 1, F32(factor), F32(1.0))
        bit *= 2
    return result


def turned(block, cosine, sine):
    block = block.astype(F32)
    return (block * cosine + pltpu.roll(block, HD // 2, 1) * sine).astype(BF16)


def kernel(
    count, hops, q_ref, k_ref, v_ref, seg_ref, out_ref,
    q_own, kwin, vwin, segwin, krot, qrot, weights, denoms, sines, cosines, bias,
    q_sem, seg_sem, own_sem, seg_send, seg_recv, send, recv, forward,
):
    me = lax.axis_index("ctx")
    rows = q_own.shape[0]
    span = bias.shape[2]
    group = qrot.shape[0] // HK
    windows = (kwin, vwin)

    def block(which, head, distance):
        return windows[which].at[head, pl.ds((hops - distance) * rows, rows)]

    own_copies = [
        [
            pltpu.make_async_copy(
                ref.at[0, :, pl.ds(head * HD, HD)], block(which, head, 0), own_sem.at[which, head]
            )
            for head in range(HK)
        ]
        for which, ref in enumerate((k_ref, v_ref))
    ]
    seg_copy = pltpu.make_async_copy(seg_ref, segwin.at[hops], seg_sem)
    q_copy = pltpu.make_async_copy(q_ref.at[0], q_own, q_sem)
    seg_copy.start()
    for which in range(2):
        for head in range(HK):
            own_copies[which][head].start()
    q_copy.start()

    barrier = pltpu.get_barrier_semaphore()
    for distance in range(1, hops + 1):
        @pl.when(me + distance < count)
        def _():
            pl.semaphore_signal(barrier, inc=1, device_id={"ctx": me + distance})

        @pl.when(me >= distance)
        def _():
            pl.semaphore_signal(barrier, inc=1, device_id={"ctx": me - distance})
    pl.semaphore_wait(barrier, jnp.minimum(me, hops) + jnp.minimum(count - 1 - me, hops))

    def seg_out(distance):
        return pltpu.make_async_remote_copy(
            src_ref=segwin.at[hops], dst_ref=segwin.at[hops - distance],
            send_sem=seg_send.at[distance - 1], recv_sem=seg_recv.at[distance - 1],
            device_id={"ctx": me + distance},
        )

    def block_out(which, head, distance):
        return pltpu.make_async_remote_copy(
            src_ref=block(which, head, 0), dst_ref=block(which, head, distance),
            send_sem=send.at[which, head, distance - 1], recv_sem=recv.at[which, head, distance - 1],
            device_id={"ctx": me + distance},
        )

    def block_on(which, head, distance):
        return pltpu.make_async_remote_copy(
            src_ref=block(which, head, distance), dst_ref=block(which, head, distance + 1),
            send_sem=forward.at[which, head, distance - 1], recv_sem=recv.at[which, head, distance],
            device_id={"ctx": me + 1},
        )

    def goes_out(distance):
        direct = me + distance < count
        if distance > 1:
            direct = direct & ((me + distance) % 2 == 0)
        return direct

    def goes_on(distance):
        return (me % 2 == 0) & (me >= distance) & (me + 1 < count)

    seg_copy.wait()
    for distance in range(1, hops + 1):
        @pl.when(me + distance < count)
        def _():
            seg_out(distance).start()
    for which in range(2):
        for head in range(HK):
            own_copies[which][head].wait()

            @pl.when(goes_out(1))
            def _():
                block_out(which, head, 1).start()
    for distance in range(2, hops + 1):
        @pl.when(goes_out(distance))
        def _():
            for which in range(2):
                for head in range(HK):
                    if distance == 2:
                        block_out(which, head, 1).wait_send()
                    block_out(which, head, distance).start()

    for distance in range(1, hops + 1):
        @pl.when(me < distance)
        def _():
            empty = jnp.zeros((HK, rows, HD), BF16)
            kwin[:, pl.ds((hops - distance) * rows, rows)] = empty
            vwin[:, pl.ds((hops - distance) * rows, rows)] = empty
            segwin[hops - distance] = jnp.full((1, rows), -1, jnp.int32)

    for distance in range(1, hops + 1):
        @pl.when(me >= distance)
        def _():
            seg_out(distance).wait_recv()

    freq = frequencies()
    lane = lax.broadcasted_iota(jnp.int32, (rows, LANES), 1)
    row = lax.broadcasted_iota(jnp.int32, (rows, LANES), 0)
    sign = jnp.where(lane < HD // 2, F32(-1.0), F32(1.0))
    ones = jnp.ones((LANES, LANES), BF16)
    pieces = []
    for index in range(hops + 1):
        seg_row = segwin[index].astype(F32)
        pieces += [seg_row[:, at:at + LANES] for at in range(0, rows, LANES)]
    for index in range(hops + 1):
        column = jnp.broadcast_to(segwin[index].astype(F32), (LANES, rows)).T
        smaller = jnp.zeros((rows, LANES), F32)
        for piece in pieces:
            smaller = smaller + jnp.where(piece < column, F32(1.0), F32(0.0))
        start = jnp.dot(smaller.astype(BF16), ones, preferred_element_type=F32)
        position = (row + index * rows).astype(F32) - start
        sine, cosine = sin_cos(position * freq)
        sines[index] = sine * sign
        cosines[index] = cosine
        if index == hops:
            last = (row + hops * rows).astype(F32)
            for tile in range(rows // LANES):
                mine = slice(tile * LANES, (tile + 1) * LANES)
                for at in range(0, span, LANES):
                    spot = (lane[mine] + (at + tile * LANES)).astype(F32)
                    bias[tile, :, at:at + LANES] = jnp.where(
                        (spot >= start[mine]) & (spot <= last[mine]), F32(0.0), F32(MASKED)
                    )

    q_copy.wait()

    @pl.loop(0, qrot.shape[0])
    def _(head):
        at = pl.ds(pl.multiple_of(head * HD, HD), HD)
        qrot[head] = turned(q_own[:, at], cosines[hops], sines[hops])

    scale = F32(math.log2(math.e) / math.sqrt(HD))

    def arrive(head, distance, which):
        @pl.when(me >= distance)
        def _():
            block_out(which, head, distance).wait_recv()
        if distance < hops:
            @pl.when(goes_on(distance))
            def _():
                block_on(which, head, distance).start()

    @pl.loop(0, HK)
    def _(head):
        for distance in range(1, hops + 1):
            arrive(head, distance, 0)
        for index in range(hops + 1):
            at = pl.ds(index * rows, rows)
            krot[at] = turned(kwin[head, at], cosines[index], sines[index])

        for part in range(group):
            for tile in range(rows // LANES):
                mine = slice(tile * LANES, (tile + 1) * LANES)
                seen = pl.ds(tile * LANES, span)
                scores = lax.dot_general(
                    qrot[head * group + part, mine], krot[seen], (((1,), (1,)), ((), ())),
                    preferred_element_type=F32,
                ) + bias[tile]
                top = jnp.max(scores, axis=1, keepdims=True)
                weight = jnp.exp2((scores - top) * scale)
                denoms[head * group + part, mine] = jnp.broadcast_to(
                    jnp.sum(weight, axis=1, keepdims=True), (LANES, LANES)
                )
                weights[head * group + part, mine] = weight.astype(BF16)

    for distance in range(1, hops):
        arrive(0, distance, 1)

    @pl.loop(0, HK)
    def _(head):
        @pl.when(head + 1 < HK)
        def _():
            for distance in range(1, hops):
                arrive(head + 1, distance, 1)

        arrive(head, hops, 1)

        for part in range(group):
            for tile in range(rows // LANES):
                mine = slice(tile * LANES, (tile + 1) * LANES)
                seen = pl.ds(tile * LANES, span)
                total = jnp.dot(weights[head * group + part, mine], vwin[head, seen], preferred_element_type=F32)
                at = pl.ds(pl.multiple_of((head * group + part) * HD, HD), HD)
                out_ref[0, mine, at] = (total / denoms[head * group + part, mine]).astype(BF16)

    for distance in range(1, hops + 1):
        @pl.when(me + distance < count)
        def _():
            seg_out(distance).wait_send()
        unsent = goes_out(distance)
        if distance == 1 and hops > 1:
            unsent = unsent & jnp.logical_not(goes_out(2))
        for which in range(2):
            for head in range(HK):
                @pl.when(unsent)
                def _():
                    block_out(which, head, distance).wait_send()
                if distance < hops:
                    @pl.when(goes_on(distance))
                    def _():
                        block_on(which, head, distance).wait_send()


def body(queries, keys, values, segments):
    count = lax.axis_size("ctx")
    hops = count // 2
    rows = queries.shape[1]
    width = (hops + 1) * rows
    span = hops * rows + LANES
    heads = queries.shape[2] // HD
    group = heads // HK
    anywhere = pl.BlockSpec(memory_space=pltpu.HBM)
    dma = pltpu.SemaphoreType.DMA
    return pl.pallas_call(
        functools.partial(kernel, count, hops),
        out_shape=pltpu.VMEM(queries.shape, BF16),
        in_specs=[anywhere] * 4,
        out_specs=pl.BlockSpec(memory_space=pltpu.VMEM),
        scratch_shapes=[
            pltpu.VMEM((rows, heads * HD), BF16),
            pltpu.VMEM((HK, width, HD), BF16),
            pltpu.VMEM((HK, width, HD), BF16),
            pltpu.VMEM((hops + 1, 1, rows), jnp.int32),
            pltpu.VMEM((width, HD), BF16),
            pltpu.VMEM((heads, rows, HD), BF16),
            pltpu.VMEM((heads, rows, span), BF16),
            pltpu.VMEM((heads, rows, LANES), F32),
            pltpu.VMEM((hops + 1, rows, HD), F32),
            pltpu.VMEM((hops + 1, rows, HD), F32),
            pltpu.VMEM((rows // LANES, LANES, span), F32),
            dma, dma, dma((2, HK)),
            dma((hops,)), dma((hops,)),
            dma((2, HK, hops)), dma((2, HK, hops)), dma((2, HK, hops)),
        ],
        compiler_params=pltpu.CompilerParams(
            collective_id=0, has_side_effects=True, vmem_limit_bytes=60 * 1024 * 1024
        ),
        name="attend",
    )(queries, keys, values, segments)


def solution(mesh):
    placed = (P("dp", "ctx", None), P("dp", "ctx", None), P("dp", "ctx", None), P("dp", "ctx"))
    return jax.shard_map(
        body, mesh=mesh, in_specs=placed, out_specs=P("dp", "ctx", None), check_vma=False
    )
```

```python
import functools
import math

import jax
import jax.numpy as jnp
from jax import lax
from jax.experimental import pallas as pl
from jax.experimental.pallas import tpu as pltpu
from jax.sharding import PartitionSpec as P

HK = 4
HD = 128
THETA = 500000.0
LANES = 128
MASKED = -1e30
F32 = jnp.float32
BF16 = jnp.bfloat16


def sin_cos(angle):
    turns = jnp.floor(angle * (2.0 / math.pi) + 0.5)
    rest = angle - turns * 1.5703125
    rest = rest - turns * 4.837512969970703125e-4
    rest = rest - turns * 7.54978995489188216e-8
    square = rest * rest
    sine = rest + rest * square * (
        -1.6666654611e-1 + square * (8.3321608736e-3 + square * -1.9515295891e-4)
    )
    cosine = (
        1.0
        - 0.5 * square
        + square * square * (4.166664568298827e-2 + square * (-1.388731625493765e-3 + square * 2.443315711809948e-5))
    )
    quarter = turns - 4.0 * jnp.floor(turns * 0.25)
    odd = (quarter == 1.0) | (quarter == 3.0)
    sin_out = jnp.where(odd, cosine, sine)
    cos_out = jnp.where(odd, sine, cosine)
    sin_out = jnp.where(quarter >= 2.0, -sin_out, sin_out)
    cos_out = jnp.where((quarter == 1.0) | (quarter == 2.0), -cos_out, cos_out)
    return sin_out, cos_out


def frequencies():
    index = lax.broadcasted_iota(jnp.int32, (1, HD), 1) % (HD // 2)
    result = jnp.ones((1, HD), F32)
    bit = 1
    while bit < HD // 2:
        factor = math.exp(-math.log(THETA) * 2.0 * bit / HD)
        result = result * jnp.where((index // bit) % 2 == 1, F32(factor), F32(1.0))
        bit *= 2
    return result


def turned(block, cosine, sine):
    block = block.astype(F32)
    return (block * cosine + pltpu.roll(block, HD // 2, 1) * sine).astype(BF16)


def kernel(
    count, hops, q_ref, k_ref, v_ref, seg_ref, out_ref,
    q_own, kwin, vwin, segwin, krot, qrot, weights, denoms, sines, cosines, bias,
    q_sem, seg_sem, own_sem, seg_send, seg_recv, send, recv, forward,
):
    me = lax.axis_index("ctx")
    rows = q_own.shape[0]
    span = bias.shape[2]
    group = qrot.shape[0] // HK
    windows = (kwin, vwin)

    def block(which, head, distance):
        return windows[which].at[head, pl.ds((hops - distance) * rows, rows)]

    own_copies = [
        [
            pltpu.make_async_copy(
                ref.at[0, :, pl.ds(head * HD, HD)], block(which, head, 0), own_sem.at[which, head]
            )
            for head in range(HK)
        ]
        for which, ref in enumerate((k_ref, v_ref))
    ]
    seg_copy = pltpu.make_async_copy(seg_ref, segwin.at[hops], seg_sem)
    q_copy = pltpu.make_async_copy(q_ref.at[0], q_own, q_sem)
    seg_copy.start()
    for which in range(2):
        for head in range(HK):
            own_copies[which][head].start()
    q_copy.start()

    barrier = pltpu.get_barrier_semaphore()
    for distance in range(1, hops + 1):
        @pl.when(me + distance < count)
        def _():
            pl.semaphore_signal(barrier, inc=1, device_id={"ctx": me + distance})

        @pl.when(me >= distance)
        def _():
            pl.semaphore_signal(barrier, inc=1, device_id={"ctx": me - distance})
    pl.semaphore_wait(barrier, jnp.minimum(me, hops) + jnp.minimum(count - 1 - me, hops))

    def seg_out(distance):
        return pltpu.make_async_remote_copy(
            src_ref=segwin.at[hops], dst_ref=segwin.at[hops - distance],
            send_sem=seg_send.at[distance - 1], recv_sem=seg_recv.at[distance - 1],
            device_id={"ctx": me + distance},
        )

    def block_out(which, head, distance):
        return pltpu.make_async_remote_copy(
            src_ref=block(which, head, 0), dst_ref=block(which, head, distance),
            send_sem=send.at[which, head, distance - 1], recv_sem=recv.at[which, head, distance - 1],
            device_id={"ctx": me + distance},
        )

    def block_on(which, head, distance):
        return pltpu.make_async_remote_copy(
            src_ref=block(which, head, distance), dst_ref=block(which, head, distance + 1),
            send_sem=forward.at[which, head, distance - 1], recv_sem=recv.at[which, head, distance],
            device_id={"ctx": me + 1},
        )

    def goes_out(distance):
        direct = me + distance < count
        if distance > 1:
            direct = direct & ((me + distance) % 2 == 0)
        return direct

    def goes_on(distance):
        return (me % 2 == 0) & (me >= distance) & (me + 1 < count)

    seg_copy.wait()
    for distance in range(1, hops + 1):
        @pl.when(me + distance < count)
        def _():
            seg_out(distance).start()
    for which in range(2):
        for head in range(HK):
            own_copies[which][head].wait()

            @pl.when(goes_out(1))
            def _():
                block_out(which, head, 1).start()
    for distance in range(2, hops + 1):
        @pl.when(goes_out(distance))
        def _():
            if distance == 2:
                for which in range(2):
                    for head in range(HK):
                        block_out(which, head, 1).wait_send()
            for which in range(2):
                for head in range(HK):
                    block_out(which, head, distance).start()

    for distance in range(1, hops + 1):
        @pl.when(me < distance)
        def _():
            empty = jnp.zeros((HK, rows, HD), BF16)
            kwin[:, pl.ds((hops - distance) * rows, rows)] = empty
            vwin[:, pl.ds((hops - distance) * rows, rows)] = empty
            segwin[hops - distance] = jnp.full((1, rows), -1, jnp.int32)

    for distance in range(1, hops + 1):
        @pl.when(me >= distance)
        def _():
            seg_out(distance).wait_recv()

    freq = frequencies()
    lane = lax.broadcasted_iota(jnp.int32, (rows, LANES), 1)
    row = lax.broadcasted_iota(jnp.int32, (rows, LANES), 0)
    sign = jnp.where(lane < HD // 2, F32(-1.0), F32(1.0))
    ones = jnp.ones((LANES, LANES), BF16)
    pieces = []
    for index in range(hops + 1):
        seg_row = segwin[index].astype(F32)
        pieces += [seg_row[:, at:at + LANES] for at in range(0, rows, LANES)]
    for index in range(hops + 1):
        column = jnp.broadcast_to(segwin[index].astype(F32), (LANES, rows)).T
        smaller = jnp.zeros((rows, LANES), F32)
        for piece in pieces:
            smaller = smaller + jnp.where(piece < column, F32(1.0), F32(0.0))
        start = jnp.dot(smaller.astype(BF16), ones, preferred_element_type=F32)
        position = (row + index * rows).astype(F32) - start
        sine, cosine = sin_cos(position * freq)
        sines[index] = sine * sign
        cosines[index] = cosine
        if index == hops:
            last = (row + hops * rows).astype(F32)
            for tile in range(rows // LANES):
                mine = slice(tile * LANES, (tile + 1) * LANES)
                for at in range(0, span, LANES):
                    spot = (lane[mine] + (at + tile * LANES)).astype(F32)
                    bias[tile, :, at:at + LANES] = jnp.where(
                        (spot >= start[mine]) & (spot <= last[mine]), F32(0.0), F32(MASKED)
                    )

    q_copy.wait()

    @pl.loop(0, qrot.shape[0])
    def _(head):
        at = pl.ds(pl.multiple_of(head * HD, HD), HD)
        qrot[head] = turned(q_own[:, at], cosines[hops], sines[hops])

    scale = F32(math.log2(math.e) / math.sqrt(HD))

    def arrive(head, distance, which):
        @pl.when(me >= distance)
        def _():
            block_out(which, head, distance).wait_recv()
        if distance < hops:
            @pl.when(goes_on(distance))
            def _():
                block_on(which, head, distance).start()

    @pl.loop(0, HK)
    def _(head):
        for distance in range(1, hops + 1):
            arrive(head, distance, 0)
        for index in range(hops + 1):
            at = pl.ds(index * rows, rows)
            krot[at] = turned(kwin[head, at], cosines[index], sines[index])

        for part in range(group):
            for tile in range(rows // LANES):
                mine = slice(tile * LANES, (tile + 1) * LANES)
                seen = pl.ds(tile * LANES, span)
                scores = lax.dot_general(
                    qrot[head * group + part, mine], krot[seen], (((1,), (1,)), ((), ())),
                    preferred_element_type=F32,
                ) + bias[tile]
                top = jnp.max(scores, axis=1, keepdims=True)
                weight = jnp.exp2((scores - top) * scale)
                denoms[head * group + part, mine] = jnp.broadcast_to(
                    jnp.sum(weight, axis=1, keepdims=True), (LANES, LANES)
                )
                weights[head * group + part, mine] = weight.astype(BF16)

    for distance in range(1, hops):
        arrive(0, distance, 1)

    @pl.loop(0, HK)
    def _(head):
        @pl.when(head + 1 < HK)
        def _():
            for distance in range(1, hops):
                arrive(head + 1, distance, 1)

        arrive(head, hops, 1)

        for part in range(group):
            for tile in range(rows // LANES):
                mine = slice(tile * LANES, (tile + 1) * LANES)
                seen = pl.ds(tile * LANES, span)
                total = jnp.dot(weights[head * group + part, mine], vwin[head, seen], preferred_element_type=F32)
                at = pl.ds(pl.multiple_of((head * group + part) * HD, HD), HD)
                out_ref[0, mine, at] = (total / denoms[head * group + part, mine]).astype(BF16)

    for distance in range(1, hops + 1):
        @pl.when(me + distance < count)
        def _():
            seg_out(distance).wait_send()
        unsent = goes_out(distance)
        if distance == 1 and hops > 1:
            unsent = unsent & jnp.logical_not(goes_out(2))
        for which in range(2):
            for head in range(HK):
                @pl.when(unsent)
                def _():
                    block_out(which, head, distance).wait_send()
                if distance < hops:
                    @pl.when(goes_on(distance))
                    def _():
                        block_on(which, head, distance).wait_send()


def body(queries, keys, values, segments):
    count = lax.axis_size("ctx")
    hops = count // 2
    rows = queries.shape[1]
    width = (hops + 1) * rows
    span = hops * rows + LANES
    heads = queries.shape[2] // HD
    group = heads // HK
    anywhere = pl.BlockSpec(memory_space=pltpu.HBM)
    dma = pltpu.SemaphoreType.DMA
    return pl.pallas_call(
        functools.partial(kernel, count, hops),
        out_shape=pltpu.VMEM(queries.shape, BF16),
        in_specs=[anywhere] * 4,
        out_specs=pl.BlockSpec(memory_space=pltpu.VMEM),
        scratch_shapes=[
            pltpu.VMEM((rows, heads * HD), BF16),
            pltpu.VMEM((HK, width, HD), BF16),
            pltpu.VMEM((HK, width, HD), BF16),
            pltpu.VMEM((hops + 1, 1, rows), jnp.int32),
            pltpu.VMEM((width, HD), BF16),
            pltpu.VMEM((heads, rows, HD), BF16),
            pltpu.VMEM((heads, rows, span), BF16),
            pltpu.VMEM((heads, rows, LANES), F32),
            pltpu.VMEM((hops + 1, rows, HD), F32),
            pltpu.VMEM((hops + 1, rows, HD), F32),
            pltpu.VMEM((rows // LANES, LANES, span), F32),
            dma, dma, dma((2, HK)),
            dma((hops,)), dma((hops,)),
            dma((2, HK, hops)), dma((2, HK, hops)), dma((2, HK, hops)),
        ],
        compiler_params=pltpu.CompilerParams(
            collective_id=0, has_side_effects=True, vmem_limit_bytes=60 * 1024 * 1024
        ),
        name="attend",
    )(queries, keys, values, segments)


def solution(mesh):
    placed = (P("dp", "ctx", None), P("dp", "ctx", None), P("dp", "ctx", None), P("dp", "ctx"))
    return jax.shard_map(
        body, mesh=mesh, in_specs=placed, out_specs=P("dp", "ctx", None), check_vma=False
    )
```
